32 devices in a mesh: group: 2 (over x), tensor: 16 (over z, y, core).
Axes of the slice: x: 2, y: 2, z: 4, core: 2. Of those that a mesh axis runs over, the one named last changes fastest.
Arguments:
- z_star: bfloat16 [64, 5120], P(('group', 'tensor')), parts along dimension 0, may hold values from -6 to 6
- grad_out: float32 [64, 5120], P(('group', 'tensor')), parts along dimension 0, may hold values from -30 to 30
- w_gate: bfloat16 [10240, 13824], P('group', 'tensor'), parts along dimension 0, may hold values from -0.078125 to 0.078125
- w_up: bfloat16 [10240, 13824], P('group', 'tensor'), parts along dimension 0, may hold values from -0.078125 to 0.078125
- w_down: bfloat16 [27648, 5120], P(('group', 'tensor')), parts along dimension 0, may hold values from -0.0546875 to 0.0546875
- norm_gain: float32 [10240], P('group'), parts along dimension 0, may hold values from 0.5 to 1.5
- mix_rate: float32 [10240], P('group'), parts along dimension 0, may hold values from 0.3 to 1
Outputs:
- adjoint: float32 [64, 5120], P(('group', 'tensor')), parts along dimension 0
- grad_gate: bfloat16 [10240, 13824], P('group', 'tensor'), parts along dimension 0
- grad_up: bfloat16 [10240, 13824], P('group', 'tensor'), parts along dimension 0
- grad_down: bfloat16 [27648, 5120], P(('group', 'tensor')), parts along dimension 0
The draws below stay inside these ranges and needn't reach their ends.
There are 2 independent parts, one for each index of `group`. The reference program is written for one: setup_inputs(seed, part) draws one part's arguments, and reference() takes and returns one part's arrays. A program takes and returns all parts, laid end to end along the dimension named above; each array names one. Nothing has to cross between parts.
All inputs are finite; a program needn't handle non-finite values.
Results may differ from the reference program's by a relative error of at most 0.014.
Values may be sent and summed in bfloat16 or wider, within the bound.
No kernel may reach another device: no remote copies, remote signals or barrier semaphores. Data moves between devices by JAX's collectives and lax.ppermute only.
A program may use at most 128 MiB of HBM per device.

```python
import math
import jax
import jax.numpy as jnp
from jax import lax

D = 5120
FF = 13824
TOKENS = 32


def draw_grad_out(key, part):
    first_key = jax.random.fold_in(key, 0)
    position = jnp.arange(TOKENS, dtype=jnp.float32) / (TOKENS - 1)
    rising = 0.6 * 3.0 ** position
    values = jax.random.normal(first_key, (TOKENS, D), jnp.float32)
    return jnp.clip(values * rising[:, None], -30.0, 30.0).astype(jnp.float32)


def steps_of(stream_key, dims, cuts, smallest, largest):
    gain, own = 1.0, jax.random.fold_in(stream_key, 6)
    for axis_at, blocks in cuts:
        draws = jnp.exp(jax.random.uniform(jax.random.fold_in(own, axis_at), (blocks,), jnp.float32, smallest / len(cuts), largest / len(cuts)))
        gain = gain * jnp.repeat(draws, dims[axis_at] // blocks).reshape([-1 if axis == axis_at else 1 for axis in range(len(dims))])
    return gain


def noise(own_key, shape, spread, bound, shards=(), kind=jnp.bfloat16):
    drawn = jax.random.normal(own_key, shape, jnp.float32) * spread
    if len(shards) > 0:
        drawn = steps_of(own_key, shape, shards, -0.22, 0.18) * drawn
    return jnp.clip(drawn, min=-bound, max=bound).astype(kind)


def setup_inputs(seed: int = 0, part: int = 0) -> dict:
    arg_keys = jax.random.split(jax.random.key(seed), 8)
    part_keys = jax.random.split(jax.random.fold_in(arg_keys[7], part), 8)
    return {
        "z_star": noise(part_keys[0], (TOKENS, D), 1.0, 6.0, ((0, 16),)),
        "grad_out": draw_grad_out(jax.random.fold_in(jax.random.fold_in(arg_keys[7], part), 71), part),
        "w_gate": noise(part_keys[2], (D, FF), D ** -0.5, 0.078125, ((1, 16),)),
        "w_up": noise(part_keys[3], (D, FF), D ** -0.5, 0.078125, ((1, 16),)),
        "w_down": noise(part_keys[4], (FF, D), FF ** -0.5, 0.0546875, ((0, 16),)),
        "norm_gain": jnp.clip(1.0 + 0.1 * jax.random.normal(part_keys[5], (D,), jnp.float32), 0.5, 1.5),
        "mix_rate": jnp.clip(jnp.exp(jax.random.uniform(part_keys[6], (D,), jnp.float32, math.log(0.3), math.log(1.0))), 0.3, 1.0),
    }


def contract(left, right, left_dim, right_dim):
    return lax.dot_general(left, right, (((left_dim,), (right_dim,)), ((), ())), preferred_element_type=jnp.float32)

def normalize(z_rows, norm_gain):
    values = z_rows.astype(jnp.float32)
    root_mean = jnp.sqrt(lax.optimization_barrier(jnp.mean(values * values, axis=-1, keepdims=True)) + 1e-06)
    unit_rows = values / root_mean
    normed = (unit_rows * norm_gain).astype(jnp.bfloat16)
    return (root_mean, unit_rows, normed)

def reference(z_star, grad_out, w_gate, w_up, w_down, norm_gain, mix_rate):
    root_mean, unit_rows, normed = normalize(z_star, norm_gain)
    gate_pre = contract(normed, w_gate, 1, 0)
    lifted = contract(normed, w_up, 1, 0)
    sigma = jax.nn.sigmoid(gate_pre)
    gated = gate_pre * sigma
    slope = sigma * (1.0 + gate_pre * (1.0 - sigma))

    def branch_grads(state):
        hidden_grad = contract(state.astype(jnp.bfloat16), w_down, 1, 1)
        gate_grad = (hidden_grad * lifted * slope).astype(jnp.bfloat16)
        lift_grad = (hidden_grad * gated).astype(jnp.bfloat16)
        return (gate_grad, lift_grad)

    def jacobian(state):
        gate_grad, lift_grad = branch_grads(state)
        normed_grad = contract(gate_grad, w_gate, 1, 1) + contract(lift_grad, w_up, 1, 1)
        scaled = norm_gain * normed_grad
        return (scaled - unit_rows * lax.optimization_barrier(jnp.mean(scaled * unit_rows, axis=-1, keepdims=True))) / root_mean
    state_zero = grad_out
    resid_zero = jacobian(state_zero)
    state_one = state_zero + mix_rate * resid_zero
    resid_one = grad_out + jacobian(state_one) - state_one
    resid_diff = resid_one - resid_zero
    blend = jnp.sum(resid_one * resid_diff) / (jnp.sum(resid_diff * resid_diff) + 1e-06)
    adjoint = state_one - blend * (state_one - state_zero) + mix_rate * (resid_one - blend * resid_diff)
    hidden = (gated * lifted).astype(jnp.bfloat16)
    adjoint_half = adjoint.astype(jnp.bfloat16)
    grad_down = contract(hidden, adjoint_half, 0, 0).astype(jnp.bfloat16)
    gate_grad, lift_grad = branch_grads(adjoint)
    grad_gate = contract(normed, gate_grad, 0, 0).astype(jnp.bfloat16)
    grad_up = contract(normed, lift_grad, 0, 0).astype(jnp.bfloat16)
    return (adjoint, grad_gate, grad_up, grad_down)
```

```python
import functools

import jax
import jax.numpy as jnp
from jax import lax
from jax.experimental import pallas as pl
from jax.experimental.pallas import tpu as pltpu
from jax.sharding import PartitionSpec as P

F32 = jnp.float32
BF16 = jnp.bfloat16
VMEM = pl.BlockSpec(memory_space=pltpu.VMEM)
HBM = pl.BlockSpec(memory_space=pltpu.HBM)
AXIS = "tensor"
ROWS = 256
LANES = 640
PLACES = 6


def dot_nn(left, right):
    return lax.dot_general(left, right, (((1,), (0,)), ((), ())), preferred_element_type=F32)


def dot_nt(left, right):
    return lax.dot_general(left, right, (((1,), (1,)), ((), ())), preferred_element_type=F32)


def dot_tn(left, right):
    return lax.dot_general(left, right, (((0,), (0,)), ((), ())), preferred_element_type=F32)


def pieces(total, size):
    return [(at, min(size, total - at)) for at in range(0, total, size)]


def lane_chunk(width):
    for size in (LANES, 512, 384, 256, 128):
        if width % size == 0:
            return size
    return width


def gather_stages(n):
    bits = [1 << k for k in reversed(range(2, n.bit_length() - 1))]
    stages = []
    while bits:
        stages.append(tuple(reversed(bits[:2])))
        bits = bits[2:]
    return stages + [(2,)]


def state_rows(slots_a, slots_b, n, me, owner):
    offset = jnp.bitwise_xor(me, owner)
    place, stride = 0, 1
    for stage in gather_stages(n):
        place = place + stride * ((offset // stage[0]) & (2 ** len(stage) - 1))
        stride *= 2 ** len(stage)
    return jnp.where((offset & 1) == 0, slots_a[place], slots_b[place])


def own_rows(ref, me, local):
    if local % 8 == 0:
        return ref[pl.ds(pl.multiple_of(me * local, 8), local), :]
    per = 8 // local
    block = ref[pl.ds(pl.multiple_of((me // per) * 8, 8), 8), :]
    value = block[:local]
    for other in range(1, per):
        value = jnp.where(me % per == other, block[other * local : (other + 1) * local], value)
    return value


def back_project(gate_grad, lift_grad, weights, ff, width, quarter, me, keep, send):
    for slot in (1, 3, 0, 2):
        at = pl.multiple_of(jnp.bitwise_xor(me & 3, slot) * quarter, 128)
        columns = pl.ds(at, quarter)
        value = dot_nn(gate_grad, weights[0:ff, columns]) + dot_nn(
            lift_grad, weights[ff : 2 * ff, columns]
        )
        target = send if slot & 1 else keep
        target[slot >> 1] = value.astype(BF16)


def first_kernel(
    n, slots_a, slots_b, gain, w_gate, w_up, w_down,
    keep, send, weights, down, z_abs, g_abs, inv, scale_gate, scale_lift, hidden, normed,
    z_rows, g_rows, gate_pre, lifted, hgrad, sems,
):
    me = lax.axis_index(AXIS)
    tokens, width = z_rows.shape
    ff = lifted.shape[1]
    local = tokens // n
    copies = []
    held = (weights.at[pl.ds(0, ff), :], weights.at[pl.ds(ff, ff), :], down)
    for index, source in enumerate((w_gate, w_up, w_down)):
        for order, (at, size) in enumerate(pieces(ff, ROWS)):
            copy = pltpu.make_async_copy(
                source.at[pl.ds(at, size), :],
                held[index].at[pl.ds(at, size), :],
                sems.at[index, order],
            )
            copy.start()
            copies.append(copy)

    for owner in range(n):
        block = state_rows(slots_a, slots_b, n, me, owner).astype(F32)
        z_rows[owner * local : (owner + 1) * local, :] = block[:local]
        g_rows[owner * local : (owner + 1) * local, :] = block[local:]

    chunk = lane_chunk(width)
    total = jnp.zeros((tokens, 1), F32)
    for at in range(0, width, chunk):
        z = z_rows[:, at : at + chunk]
        total = total + jnp.sum(z * z, axis=1, keepdims=True)
        z_abs[:, at : at + chunk] = z.astype(BF16)
        g_abs[:, at : at + chunk] = g_rows[:, at : at + chunk].astype(BF16)
    inverse = 1.0 / jnp.sqrt(total / width + 1e-06)
    inv[...] = jnp.broadcast_to(inverse, inv.shape)
    for at in range(0, width, chunk):
        unit = z_rows[:, at : at + chunk] * inverse
        normed[:, at : at + chunk] = (unit * gain[:, at : at + chunk]).astype(BF16)

    rows = pieces(ff, ROWS)
    for index, target in enumerate((gate_pre, lifted, hgrad)):
        left = g_abs if index == 2 else normed
        for order, (at, size) in enumerate(rows):
            copies[index * len(rows) + order].wait()
            target[:, at : at + size] = dot_nt(left[...], held[index][at : at + size, :])

    pre = gate_pre[...]
    up = lifted[...]
    sigma = 1.0 / (1.0 + jnp.exp(-pre))
    gated = pre * sigma
    slope = sigma * (1.0 + pre * (1.0 - sigma))
    by_gate = up * slope
    scale_gate[...] = by_gate
    scale_lift[...] = gated
    hidden[...] = (gated * up).astype(BF16)
    grad = hgrad[...]
    back_project(
        (grad * by_gate).astype(BF16), (grad * gated).astype(BF16),
        weights, ff, width, width // 4, me, keep, send,
    )


def scaled_rows(me, slots, z_abs, gain, inverse, scaled):
    quarter = slots[0].shape[-1]
    tokens, width = scaled.shape
    chunk = lane_chunk(quarter)
    total = jnp.zeros((tokens, 1), F32)
    for slot, source in enumerate(slots):
        base = jnp.bitwise_xor(me & 3, slot) * quarter
        for at in range(0, quarter, chunk):
            columns = pl.ds(pl.multiple_of(base + at, 128), chunk)
            value = source[:, at : at + chunk].astype(F32) * gain[:, columns]
            scaled[:, columns] = value
            unit = z_abs[:, columns].astype(F32) * inverse
            total = total + jnp.sum(value * unit, axis=1, keepdims=True)
    return total / width


def second_kernel(
    slot_0, slot_1, slot_2, slot_3, z_abs, g_abs, inv, gain, mix, scale_gate, scale_lift, weights, down,
    keep, send, resid,
    scaled, state, hgrad,
):
    me = lax.axis_index(AXIS)
    tokens, width = scaled.shape
    ff = hgrad.shape[1]
    inverse = inv[:, 0:1]
    mean = scaled_rows(me, (slot_0, slot_1, slot_2, slot_3), z_abs, gain, inverse, scaled)
    chunk = lane_chunk(width)
    for at in range(0, width, chunk):
        columns = slice(at, at + chunk)
        unit = z_abs[:, columns].astype(F32) * inverse
        back = (scaled[:, columns] - unit * mean) * inverse
        resid[:, columns] = back
        state[:, columns] = (g_abs[:, columns].astype(F32) + mix[:, columns] * back).astype(BF16)
    for at, size in pieces(ff, ROWS):
        hgrad[:, at : at + size] = dot_nt(state[...], down[at : at + size, :])
    grad = hgrad[...]
    back_project(
        (grad * scale_gate[...]).astype(BF16), (grad * scale_lift[...]).astype(BF16),
        weights, ff, width, width // 4, me, keep, send,
    )


def third_kernel(
    n, slot_0, slot_1, slot_2, slot_3, z_abs, g_abs, inv, gain, mix, scale_gate, scale_lift,
    down, resid, hidden, normed,
    adjoint, d_gate, d_up, d_down,
    scaled, latest, half, hgrad, stage, sems,
):
    me = lax.axis_index(AXIS)
    tokens, width = scaled.shape
    ff = hgrad.shape[1]
    local = tokens // n
    inverse = inv[:, 0:1]
    mean = scaled_rows(me, (slot_0, slot_1, slot_2, slot_3), z_abs, gain, inverse, scaled)
    chunk = lane_chunk(width)
    cross = jnp.zeros((tokens, 1), F32)
    square = jnp.zeros((tokens, 1), F32)
    for at in range(0, width, chunk):
        columns = slice(at, at + chunk)
        unit = z_abs[:, columns].astype(F32) * inverse
        back = (scaled[:, columns] - unit * mean) * inverse
        start = g_abs[:, columns].astype(F32)
        before = resid[:, columns]
        state = start + mix[:, columns] * before
        now = start + back - state
        change = now - before
        latest[:, columns] = now
        cross = cross + jnp.sum(now * change, axis=1, keepdims=True)
        square = square + jnp.sum(change * change, axis=1, keepdims=True)
    blend = jnp.sum(cross, axis=0, keepdims=True) / (
        jnp.sum(square, axis=0, keepdims=True) + 1e-06
    )
    for at in range(0, width, chunk):
        columns = slice(at, at + chunk)
        start = g_abs[:, columns].astype(F32)
        before = resid[:, columns]
        rate = mix[:, columns]
        state = start + rate * before
        now = latest[:, columns]
        value = state - blend * (state - start) + rate * (now - blend * (now - before))
        scaled[:, columns] = value
        half[:, columns] = value.astype(BF16)
    adjoint[...] = own_rows(scaled, me, local)

    places, _, step = stage.shape
    copies = []

    def emit(left, right, target, at):
        place = len(copies) % places
        if len(copies) >= places:
            copies[-places].wait()
        stage[place] = dot_tn(left, right[:, at : at + step]).astype(BF16)
        copy = pltpu.make_async_copy(
            stage.at[place], target.at[:, pl.ds(at, step)], sems.at[place]
        )
        copy.start()
        copies.append(copy)

    for at in range(0, width, step):
        emit(hidden[...], half, d_down, at)
    for at, size in pieces(ff, ROWS):
        hgrad[:, at : at + size] = dot_nt(half[...], down[at : at + size, :])
    grad = hgrad[...]
    gate_grad = (grad * scale_gate[...]).astype(BF16)
    lift_grad = (grad * scale_lift[...]).astype(BF16)
    for at in range(0, width, step):
        emit(gate_grad, normed, d_gate, at)
        emit(lift_grad, normed, d_up, at)
    for copy in copies[-places:]:
        copy.wait()


def shape(dims, dtype):
    return jax.ShapeDtypeStruct(dims, dtype)


def in_hbm(array):
    return pltpu.with_memory_space_constraint(array, pltpu.HBM)


def params(state_bytes, extra=0):
    return pltpu.CompilerParams(vmem_limit_bytes=6 * 2**20 + 6 * state_bytes + extra)


def cost(flops, moved):
    return pl.CostEstimate(flops=flops, bytes_accessed=moved, transcendentals=0)


def exchange(value, n, bit):
    return lax.ppermute(value, AXIS, [(i, i ^ bit) for i in range(n)])


def add(*terms):
    total = terms[0].astype(F32)
    for term in terms[1:]:
        total = total + term.astype(F32)
    return total.astype(BF16)


def gather_slots(own, n):
    held = own[None]
    for stage in gather_stages(n):
        steps = stage if len(stage) == 1 else (stage[0], stage[1], stage[0] + stage[1])
        held = jnp.concatenate([held] + [exchange(held, n, step) for step in steps], axis=0)
    return held, exchange(held, n, 1)


def sum_everywhere(keep, send, n):
    both = add(keep, exchange(send, n, 1))
    own = add(both[0], exchange(both[1], n, 2))
    bit = 4
    while bit < n:
        own = add(own, exchange(own, n, bit))
        bit *= 2
    beside = exchange(own, n, 2)
    return own, exchange(own, n, 1), beside, exchange(beside, n, 1)


def body(n, z_star, grad_out, w_gate, w_up, w_down, norm_gain, mix_rate):
    local, width = z_star.shape
    ff = w_gate.shape[1]
    tokens = local * n
    quarter = width // 4
    gain, mix = norm_gain[None], mix_rate[None]
    packed = jnp.concatenate([z_star, grad_out.astype(BF16)], axis=0)
    slots_a, slots_b = gather_slots(packed, n)
    chunks = len(pieces(ff, ROWS))
    partial = shape((2, tokens, quarter), BF16)
    mat = 2 * tokens * width * ff

    outs = pl.pallas_call(
        functools.partial(first_kernel, n),
        out_shape=(
            partial, partial, shape((2 * ff, width), BF16), shape((ff, width), BF16), shape((tokens, width), BF16),
            shape((tokens, width), BF16), shape((tokens, 128), F32), shape((tokens, ff), F32),
            shape((tokens, ff), F32), shape((tokens, ff), BF16), shape((tokens, width), BF16),
        ),
        in_specs=[VMEM] * 3 + [HBM] * 3,
        out_specs=(VMEM,) * 11,
        scratch_shapes=[
            pltpu.VMEM((tokens, width), F32), pltpu.VMEM((tokens, width), F32),
            pltpu.VMEM((tokens, ff), F32), pltpu.VMEM((tokens, ff), F32), pltpu.VMEM((tokens, ff), F32),
            pltpu.SemaphoreType.DMA((3, chunks)),
        ],
        compiler_params=params(4 * tokens * width),
        cost_estimate=cost(5 * mat, 3 * ff * width * 2),
        name="forward_first",
    )(slots_a, slots_b, gain, in_hbm(w_gate.T), in_hbm(w_up.T), in_hbm(w_down))

    keep, send, weights, down, z_abs, g_abs, inv, scale_gate, scale_lift, hidden, normed = outs
    slots = sum_everywhere(keep, send, n)
    keep, send, resid = pl.pallas_call(
        second_kernel,
        out_shape=(partial, partial, shape((tokens, width), F32)),
        in_specs=[VMEM] * 13,
        out_specs=(VMEM,) * 3,
        scratch_shapes=[
            pltpu.VMEM((tokens, width), F32), pltpu.VMEM((tokens, width), BF16),
            pltpu.VMEM((tokens, ff), F32),
        ],
        compiler_params=params(4 * tokens * width),
        cost_estimate=cost(3 * mat, 3 * ff * width * 2),
        name="second",
    )(*slots, z_abs, g_abs, inv, gain, mix, scale_gate, scale_lift, weights, down)

    slots = sum_everywhere(keep, send, n)
    step = 1024 if width % 1024 == 0 else lane_chunk(quarter)
    adjoint, d_gate, d_up, d_down = pl.pallas_call(
        functools.partial(third_kernel, n),
        out_shape=(
            shape((local, width), F32), shape((ff, width), BF16), shape((ff, width), BF16),
            shape((ff, width), BF16),
        ),
        in_specs=[VMEM] * 15,
        out_specs=(VMEM, HBM, HBM, HBM),
        scratch_shapes=[
            pltpu.VMEM((tokens, width), F32), pltpu.VMEM((tokens, width), F32),
            pltpu.VMEM((tokens, width), BF16), pltpu.VMEM((tokens, ff), F32),
            pltpu.VMEM((PLACES, ff, step), BF16), pltpu.SemaphoreType.DMA((PLACES,)),
        ],
        compiler_params=params(4 * tokens * width, 2 * PLACES * ff * step),
        cost_estimate=cost(4 * mat, 3 * ff * width * 2),
        name="third",
    )(*slots, z_abs, g_abs, inv, gain, mix, scale_gate, scale_lift, down, resid, hidden, normed)
    return adjoint, d_gate.T, d_up.T, d_down


def solution(mesh):
    n = mesh.shape[AXIS]
    rows = P(("group", AXIS), None)
    split = P("group", AXIS)
    placed = (rows, rows, split, split, rows, P("group"), P("group"))
    return jax.shard_map(
        functools.partial(body, n),
        mesh=mesh,
        in_specs=placed,
        out_specs=(rows, split, split, rows),
        check_vma=False,
    )
```

```python
import functools

import jax
import jax.numpy as jnp
from jax import lax
from jax.experimental import pallas as pl
from jax.experimental.pallas import tpu as pltpu
from jax.sharding import PartitionSpec as P

F32 = jnp.float32
BF16 = jnp.bfloat16
VMEM = pl.BlockSpec(memory_space=pltpu.VMEM)
HBM = pl.BlockSpec(memory_space=pltpu.HBM)
AXIS = "tensor"
ROWS = 256
LANES = 640
PLACES = 6
LOAD_FLOPS = 2 * 10**9


def dot_nn(left, right):
    return lax.dot_general(left, right, (((1,), (0,)), ((), ())), preferred_element_type=F32)


def dot_nt(left, right):
    return lax.dot_general(left, right, (((1,), (1,)), ((), ())), preferred_element_type=F32)


def dot_tn(left, right):
    return lax.dot_general(left, right, (((0,), (0,)), ((), ())), preferred_element_type=F32)


def pieces(total, size):
    return [(at, min(size, total - at)) for at in range(0, total, size)]


def lane_chunk(width):
    for size in (LANES, 512, 384, 256, 128):
        if width % size == 0:
            return size
    return width


def gather_stages(n):
    bits = [1 << k for k in reversed(range(2, n.bit_length() - 1))]
    stages = []
    while bits:
        stages.append(tuple(reversed(bits[:2])))
        bits = bits[2:]
    return stages + [(2,)]


def state_rows(slots_a, slots_b, n, me, owner):
    offset = jnp.bitwise_xor(me, owner)
    place, stride = 0, 1
    for stage in gather_stages(n):
        place = place + stride * ((offset // stage[0]) & (2 ** len(stage) - 1))
        stride *= 2 ** len(stage)
    return jnp.where((offset & 1) == 0, slots_a[place], slots_b[place])


def own_rows(ref, me, local):
    if local % 8 == 0:
        return ref[pl.ds(pl.multiple_of(me * local, 8), local), :]
    per = 8 // local
    block = ref[pl.ds(pl.multiple_of((me // per) * 8, 8), 8), :]
    value = block[:local]
    for other in range(1, per):
        value = jnp.where(me % per == other, block[other * local : (other + 1) * local], value)
    return value


def back_project(gate_grad, lift_grad, w_gate, w_up, me, keep, send):
    quarter = keep.shape[-1]
    for slot in (1, 3, 0, 2):
        at = pl.multiple_of(jnp.bitwise_xor(me & 3, slot) * quarter, 128)
        columns = pl.ds(at, quarter)
        value = dot_nn(gate_grad, w_gate[:, columns]) + dot_nn(lift_grad, w_up[:, columns])
        target = send if slot & 1 else keep
        target[slot >> 1] = value.astype(BF16)


def load_kernel(source, held, sems):
    copies = [
        pltpu.make_async_copy(source.at[pl.ds(at, size), :], held.at[pl.ds(at, size), :], sems.at[order])
        for order, (at, size) in enumerate(pieces(source.shape[0], ROWS))
    ]
    for copy in copies:
        copy.start()
    for copy in copies:
        copy.wait()


def pack_kernel(z, g, packed):
    local = z.shape[0]
    packed[0, :local] = z[...]
    packed[0, local:] = g[...].astype(BF16)


def first_kernel(
    n, slots_a, slots_b, gain_hbm, w_gate, w_up, w_down,
    keep, send, z_abs, g_abs, inv, scale_gate, scale_lift, hidden, normed,
    z_rows, g_rows, gain, gate_pre, lifted, hgrad, gain_sem,
):
    me = lax.axis_index(AXIS)
    tokens, width = z_rows.shape
    ff = lifted.shape[1]
    local = tokens // n
    gain_copy = pltpu.make_async_copy(gain_hbm, gain, gain_sem)
    gain_copy.start()
    for owner in range(n):
        block = state_rows(slots_a, slots_b, n, me, owner).astype(F32)
        z_rows[owner * local : (owner + 1) * local, :] = block[:local]
        g_rows[owner * local : (owner + 1) * local, :] = block[local:]

    chunk = lane_chunk(width)
    total = jnp.zeros((tokens, 1), F32)
    for at in range(0, width, chunk):
        z = z_rows[:, at : at + chunk]
        total = total + jnp.sum(z * z, axis=1, keepdims=True)
        z_abs[:, at : at + chunk] = z.astype(BF16)
        g_abs[:, at : at + chunk] = g_rows[:, at : at + chunk].astype(BF16)
    inverse = 1.0 / jnp.sqrt(total / width + 1e-06)
    inv[...] = jnp.broadcast_to(inverse, inv.shape)
    gain_copy.wait()
    for at in range(0, width, chunk):
        unit = z_rows[:, at : at + chunk] * inverse
        normed[:, at : at + chunk] = (unit * gain[:, at : at + chunk]).astype(BF16)

    project(normed, w_gate, gate_pre)
    project(normed, w_up, lifted)
    project(g_abs, w_down, hgrad)
    pre = gate_pre[...]
    up = lifted[...]
    sigma = 1.0 / (1.0 + jnp.exp(-pre))
    gated = pre * sigma
    slope = sigma * (1.0 + pre * (1.0 - sigma))
    by_gate = up * slope
    scale_gate[...] = by_gate
    scale_lift[...] = gated
    hidden[...] = (gated * up).astype(BF16)
    grad = hgrad[...]
    back_project(
        (grad * by_gate).astype(BF16), (grad * gated).astype(BF16),
        w_gate, w_up, me, keep, send,
    )


def project(left, weight, target):
    for at, size in pieces(weight.shape[0], ROWS):
        target[:, at : at + size] = dot_nt(left[...], weight[at : at + size, :])


def scaled_rows(me, slots, z_abs, gain, inverse, scaled):
    quarter = slots[0].shape[-1]
    tokens, width = scaled.shape
    chunk = lane_chunk(quarter)
    total = jnp.zeros((tokens, 1), F32)
    for slot, source in enumerate(slots):
        base = jnp.bitwise_xor(me & 3, slot) * quarter
        for at in range(0, quarter, chunk):
            columns = pl.ds(pl.multiple_of(base + at, 128), chunk)
            value = source[:, at : at + chunk].astype(F32) * gain[:, columns]
            scaled[:, columns] = value
            unit = z_abs[:, columns].astype(F32) * inverse
            total = total + jnp.sum(value * unit, axis=1, keepdims=True)
    return total / width


def second_kernel(
    slot_0, slot_1, slot_2, slot_3, z_abs, g_abs, inv, gain, mix, scale_gate, scale_lift, w_gate, w_up, down,
    keep, send, resid,
    scaled, state, hgrad,
):
    me = lax.axis_index(AXIS)
    tokens, width = scaled.shape
    ff = hgrad.shape[1]
    inverse = inv[:, 0:1]
    mean = scaled_rows(me, (slot_0, slot_1, slot_2, slot_3), z_abs, gain, inverse, scaled)
    chunk = lane_chunk(width)
    for at in range(0, width, chunk):
        columns = slice(at, at + chunk)
        unit = z_abs[:, columns].astype(F32) * inverse
        back = (scaled[:, columns] - unit * mean) * inverse
        resid[:, columns] = back
        state[:, columns] = (g_abs[:, columns].astype(F32) + mix[:, columns] * back).astype(BF16)
    project(state, down, hgrad)
    grad = hgrad[...]
    back_project(
        (grad * scale_gate[...]).astype(BF16), (grad * scale_lift[...]).astype(BF16),
        w_gate, w_up, me, keep, send,
    )


def third_kernel(
    n, slot_0, slot_1, slot_2, slot_3, z_abs, g_abs, inv, gain, mix, scale_gate, scale_lift,
    down, resid, hidden, normed,
    adjoint, d_gate, d_up, d_down,
    scaled, latest, half, hgrad, stage, sems,
):
    me = lax.axis_index(AXIS)
    tokens, width = scaled.shape
    ff = hgrad.shape[1]
    local = tokens // n
    inverse = inv[:, 0:1]
    mean = scaled_rows(me, (slot_0, slot_1, slot_2, slot_3), z_abs, gain, inverse, scaled)
    chunk = lane_chunk(width)
    cross = jnp.zeros((tokens, 1), F32)
    square = jnp.zeros((tokens, 1), F32)
    for at in range(0, width, chunk):
        columns = slice(at, at + chunk)
        unit = z_abs[:, columns].astype(F32) * inverse
        back = (scaled[:, columns] - unit * mean) * inverse
        start = g_abs[:, columns].astype(F32)
        before = resid[:, columns]
        state = start + mix[:, columns] * before
        now = start + back - state
        change = now - before
        latest[:, columns] = now
        cross = cross + jnp.sum(now * change, axis=1, keepdims=True)
        square = square + jnp.sum(change * change, axis=1, keepdims=True)
    blend = jnp.sum(cross, axis=0, keepdims=True) / (
        jnp.sum(square, axis=0, keepdims=True) + 1e-06
    )
    for at in range(0, width, chunk):
        columns = slice(at, at + chunk)
        start = g_abs[:, columns].astype(F32)
        before = resid[:, columns]
        rate = mix[:, columns]
        state = start + rate * before
        now = latest[:, columns]
        value = state - blend * (state - start) + rate * (now - blend * (now - before))
        scaled[:, columns] = value
        half[:, columns] = value.astype(BF16)
    adjoint[...] = own_rows(scaled, me, local)

    places, _, step = stage.shape
    copies = []

    def emit(left, right, target, at):
        place = len(copies) % places
        if len(copies) >= places:
            copies[-places].wait()
        stage[place] = dot_tn(left, right[:, at : at + step]).astype(BF16)
        copy = pltpu.make_async_copy(
            stage.at[place], target.at[:, pl.ds(at, step)], sems.at[place]
        )
        copy.start()
        copies.append(copy)

    for at in range(0, width, step):
        emit(hidden[...], half, d_down, at)
    project(half, down, hgrad)
    grad = hgrad[...]
    gate_grad = (grad * scale_gate[...]).astype(BF16)
    lift_grad = (grad * scale_lift[...]).astype(BF16)
    for at in range(0, width, step):
        emit(gate_grad, normed, d_gate, at)
        emit(lift_grad, normed, d_up, at)
    for copy in copies[-places:]:
        copy.wait()


def shape(dims, dtype):
    return jax.ShapeDtypeStruct(dims, dtype)


def in_hbm(array):
    return pltpu.with_memory_space_constraint(array, pltpu.HBM)


def params(state_bytes, extra=0):
    return pltpu.CompilerParams(vmem_limit_bytes=6 * 2**20 + 6 * state_bytes + extra)


def cost(flops, moved):
    return pl.CostEstimate(flops=flops, bytes_accessed=moved, transcendentals=0)


def exchange(value, n, bit):
    return lax.ppermute(value, AXIS, [(i, i ^ bit) for i in range(n)])


def add(*terms):
    total = terms[0].astype(F32)
    for term in terms[1:]:
        total = total + term.astype(F32)
    return total.astype(BF16)


def gather_slots(own, n, w_gate, w_up, w_down):
    sources = [(w_gate, "load_gate"), (w_up, "load_up")]
    ready = []
    held = own
    for stage in gather_stages(n):
        steps = stage if len(stage) == 1 else (stage[0], stage[1], stage[0] + stage[1])
        arrived = [exchange(held, n, step) for step in steps]
        if sources:
            source, name = sources.pop(0)
            ready.append(load(source, name))
            arrived, ready[-1], sources = hold_order(arrived, ready[-1], sources)
        held = jnp.concatenate([held] + arrived, axis=0)
    ready += [load(source, name) for source, name in sources]
    return held, exchange(held, n, 1), *ready, load(w_down, "load_down")


def hold_order(arrived, loaded, sources):
    names = [name for _, name in sources]
    arrived, loaded, arrays = lax.optimization_barrier((arrived, loaded, [array for array, _ in sources]))
    return arrived, loaded, list(zip(arrays, names))


def sum_everywhere(keep, send, n):
    both = add(keep, exchange(send, n, 1))
    own = add(both[0], exchange(both[1], n, 2))
    bit = 4
    while bit < n:
        own = add(own, exchange(own, n, bit))
        bit *= 2
    beside = exchange(own, n, 2)
    return own, exchange(own, n, 1), beside, exchange(beside, n, 1)


def pack(z_star, grad_out):
    local, width = z_star.shape
    return pl.pallas_call(
        pack_kernel,
        out_shape=shape((1, 2 * local, width), BF16),
        in_specs=[VMEM] * 2,
        out_specs=VMEM,
        compiler_params=params(0),
        name="pack",
    )(z_star, grad_out)


def load(weight, name):
    return pl.pallas_call(
        load_kernel,
        out_shape=shape(weight.shape, BF16),
        in_specs=[HBM],
        out_specs=VMEM,
        scratch_shapes=[pltpu.SemaphoreType.DMA((len(pieces(weight.shape[0], ROWS)),))],
        compiler_params=params(0),
        cost_estimate=cost(LOAD_FLOPS, 2 * weight.size),
        name=name,
    )(in_hbm(weight))


def call_first(n, slots_a, slots_b, gain, w_gate, w_up, w_down):
    _, packed, width = slots_a.shape
    tokens, ff = packed * n // 2, w_down.shape[0]
    partial = shape((2, tokens, width // 4), BF16)
    return pl.pallas_call(
        functools.partial(first_kernel, n),
        out_shape=(
            partial, partial,
            shape((tokens, width), BF16), shape((tokens, width), BF16), shape((tokens, 128), F32),
            shape((tokens, ff), F32), shape((tokens, ff), F32), shape((tokens, ff), BF16),
            shape((tokens, width), BF16),
        ),
        in_specs=[VMEM] * 2 + [HBM] + [VMEM] * 3,
        out_specs=(VMEM,) * 9,
        scratch_shapes=[
            pltpu.VMEM((tokens, width), F32), pltpu.VMEM((tokens, width), F32), pltpu.VMEM((1, width), F32),
            pltpu.VMEM((tokens, ff), F32), pltpu.VMEM((tokens, ff), F32), pltpu.VMEM((tokens, ff), F32),
            pltpu.SemaphoreType.DMA,
        ],
        compiler_params=params(4 * tokens * width),
        cost_estimate=cost(10 * tokens * width * ff, 6 * ff * width),
        name="first",
    )(slots_a, slots_b, in_hbm(gain), w_gate, w_up, w_down)


def call_second(slots, z_abs, g_abs, inv, gain, mix, scale_gate, scale_lift, w_gate, w_up, down):
    tokens, width = z_abs.shape
    ff = down.shape[0]
    partial = shape((2, tokens, width // 4), BF16)
    return pl.pallas_call(
        second_kernel,
        out_shape=(partial, partial, shape((tokens, width), F32)),
        in_specs=[VMEM] * 14,
        out_specs=(VMEM,) * 3,
        scratch_shapes=[
            pltpu.VMEM((tokens, width), F32), pltpu.VMEM((tokens, width), BF16),
            pltpu.VMEM((tokens, ff), F32),
        ],
        compiler_params=params(4 * tokens * width),
        cost_estimate=cost(6 * tokens * width * ff, 6 * ff * width),
        name="second",
    )(*slots, z_abs, g_abs, inv, gain, mix, scale_gate, scale_lift, w_gate, w_up, down)


def call_third(
    n, slots, z_abs, g_abs, inv, gain, mix, scale_gate, scale_lift, down, resid, hidden, normed
):
    tokens, width = z_abs.shape
    ff = down.shape[0]
    step = 1024 if width % 1024 == 0 else lane_chunk(width // 4)
    return pl.pallas_call(
        functools.partial(third_kernel, n),
        out_shape=(shape((tokens // n, width), F32),) + (shape((ff, width), BF16),) * 3,
        in_specs=[VMEM] * 15,
        out_specs=(VMEM, HBM, HBM, HBM),
        scratch_shapes=[
            pltpu.VMEM((tokens, width), F32), pltpu.VMEM((tokens, width), F32),
            pltpu.VMEM((tokens, width), BF16), pltpu.VMEM((tokens, ff), F32),
            pltpu.VMEM((PLACES, ff, step), BF16), pltpu.SemaphoreType.DMA((PLACES,)),
        ],
        compiler_params=params(4 * tokens * width, 2 * PLACES * ff * step),
        cost_estimate=cost(8 * tokens * width * ff, 6 * ff * width),
        name="third",
    )(*slots, z_abs, g_abs, inv, gain, mix, scale_gate, scale_lift, down, resid, hidden, normed)


def body(n, z_star, grad_out, w_gate, w_up, w_down, norm_gain, mix_rate):
    gain, mix = norm_gain[None], mix_rate[None]
    slots_a, slots_b, gate, up, down = gather_slots(pack(z_star, grad_out), n, w_gate.T, w_up.T, w_down)
    keep, send, z_abs, g_abs, inv, scale_gate, scale_lift, hidden, normed = call_first(
        n, slots_a, slots_b, gain, gate, up, down
    )
    slots = sum_everywhere(keep, send, n)
    keep, send, resid = call_second(
        slots, z_abs, g_abs, inv, gain, mix, scale_gate, scale_lift, gate, up, down
    )
    slots = sum_everywhere(keep, send, n)
    adjoint, d_gate, d_up, d_down = call_third(
        n, slots, z_abs, g_abs, inv, gain, mix, scale_gate, scale_lift, down, resid, hidden, normed
    )
    return adjoint, d_gate.T, d_up.T, d_down


def solution(mesh):
    n = mesh.shape[AXIS]
    rows = P(("group", AXIS), None)
    split = P("group", AXIS)
    placed = (rows, rows, split, split, rows, P("group"), P("group"))
    return jax.shard_map(
        functools.partial(body, n),
        mesh=mesh,
        in_specs=placed,
        out_specs=(rows, split, split, rows),
        check_vma=False,
    )
```

```python
import functools

import jax
import jax.numpy as jnp
from jax import lax
from jax.experimental import pallas as pl
from jax.experimental.pallas import tpu as pltpu
from jax.sharding import PartitionSpec as P

F32 = jnp.float32
BF16 = jnp.bfloat16
VMEM = pl.BlockSpec(memory_space=pltpu.VMEM)
HBM = pl.BlockSpec(memory_space=pltpu.HBM)
AXIS = "tensor"
ROWS = 256
LANES = 640
PLACES = 6
LOAD_FLOPS = 2 * 10**9


def dot_nn(left, right):
    return lax.dot_general(left, right, (((1,), (0,)), ((), ())), preferred_element_type=F32)


def dot_nt(left, right):
    return lax.dot_general(left, right, (((1,), (1,)), ((), ())), preferred_element_type=F32)


def dot_tn(left, right):
    return lax.dot_general(left, right, (((0,), (0,)), ((), ())), preferred_element_type=F32)


def pieces(total, size):
    return [(at, min(size, total - at)) for at in range(0, total, size)]


def lane_chunk(width):
    for size in (LANES, 512, 384, 256, 128):
        if width % size == 0:
            return size
    return width


def gather_stages(n):
    bits = [1 << k for k in reversed(range(2, n.bit_length() - 1))]
    stages = []
    while bits:
        stages.append(tuple(reversed(bits[:2])))
        bits = bits[2:]
    return stages + [(2,)]


def state_rows(slots_a, slots_b, n, me, owner):
    offset = jnp.bitwise_xor(me, owner)
    place, stride = 0, 1
    for stage in gather_stages(n):
        place = place + stride * ((offset // stage[0]) & (2 ** len(stage) - 1))
        stride *= 2 ** len(stage)
    return jnp.where((offset & 1) == 0, slots_a[place], slots_b[place])


def own_rows(ref, me, local):
    if local % 8 == 0:
        return ref[pl.ds(pl.multiple_of(me * local, 8), local), :]
    per = 8 // local
    block = ref[pl.ds(pl.multiple_of((me // per) * 8, 8), 8), :]
    value = block[:local]
    for other in range(1, per):
        value = jnp.where(me % per == other, block[other * local : (other + 1) * local], value)
    return value


def back_project(gate_grad, lift_grad, w_gate, w_up, me, keep, send):
    quarter = keep[0].shape[-1]
    for slot in (1, 3, 0, 2):
        at = pl.multiple_of(jnp.bitwise_xor(me & 1, slot) * quarter, 128)
        columns = pl.ds(at, quarter)
        value = dot_nn(gate_grad, w_gate[:, columns]) + dot_nn(lift_grad, w_up[:, columns])
        targets = send if slot & 1 else keep
        targets[slot >> 1][...] = value.astype(BF16)


def load_kernel(source, held, sems):
    copies = [
        pltpu.make_async_copy(source.at[pl.ds(at, size), :], held.at[pl.ds(at, size), :], sems.at[order])
        for order, (at, size) in enumerate(pieces(source.shape[0], ROWS))
    ]
    for copy in copies:
        copy.start()
    for copy in copies:
        copy.wait()


def pack_kernel(z, g, packed):
    local = z.shape[0]
    packed[0, :local] = z[...]
    packed[0, local:] = g[...].astype(BF16)


def first_kernel(
    n, slots_a, slots_b, gain_hbm, w_gate, w_up, w_down,
    keep_0, keep_1, send_0, send_1, z_abs, g_abs, inv, scale_gate, scale_lift, hidden, normed,
    z_rows, g_rows, gain, gate_pre, lifted, hgrad, gain_sem,
):
    me = lax.axis_index(AXIS)
    tokens, width = z_rows.shape
    ff = lifted.shape[1]
    local = tokens // n
    gain_copy = pltpu.make_async_copy(gain_hbm, gain, gain_sem)
    gain_copy.start()
    for owner in range(n):
        block = state_rows(slots_a, slots_b, n, me, owner).astype(F32)
        z_rows[owner * local : (owner + 1) * local, :] = block[:local]
        g_rows[owner * local : (owner + 1) * local, :] = block[local:]

    chunk = lane_chunk(width)
    total = jnp.zeros((tokens, 1), F32)
    for at in range(0, width, chunk):
        z = z_rows[:, at : at + chunk]
        total = total + jnp.sum(z * z, axis=1, keepdims=True)
        z_abs[:, at : at + chunk] = z.astype(BF16)
        g_abs[:, at : at + chunk] = g_rows[:, at : at + chunk].astype(BF16)
    inverse = 1.0 / jnp.sqrt(total / width + 1e-06)
    inv[...] = jnp.broadcast_to(inverse, inv.shape)
    gain_copy.wait()
    for at in range(0, width, chunk):
        unit = z_rows[:, at : at + chunk] * inverse
        normed[:, at : at + chunk] = (unit * gain[:, at : at + chunk]).astype(BF16)

    project(normed, w_gate, gate_pre)
    project(normed, w_up, lifted)
    project(g_abs, w_down, hgrad)
    pre = gate_pre[...]
    up = lifted[...]
    sigma = 1.0 / (1.0 + jnp.exp(-pre))
    gated = pre * sigma
    slope = sigma * (1.0 + pre * (1.0 - sigma))
    by_gate = up * slope
    scale_gate[...] = by_gate
    scale_lift[...] = gated
    hidden[...] = (gated * up).astype(BF16)
    grad = hgrad[...]
    back_project(
        (grad * by_gate).astype(BF16), (grad * gated).astype(BF16),
        w_gate, w_up, me, (keep_0, keep_1), (send_0, send_1),
    )


def project(left, weight, target):
    for at, size in pieces(weight.shape[0], ROWS):
        target[:, at : at + size] = dot_nt(left[...], weight[at : at + size, :])


def scaled_rows(me, slots, z_abs, gain, inverse, scaled):
    quarter = slots[0].shape[-1]
    tokens, width = scaled.shape
    chunk = lane_chunk(quarter)
    total = jnp.zeros((tokens, 1), F32)
    for slot, source in enumerate(slots):
        base = jnp.bitwise_xor(me & 1, slot) * quarter
        for at in range(0, quarter, chunk):
            columns = pl.ds(pl.multiple_of(base + at, 128), chunk)
            value = source[:, at : at + chunk].astype(F32) * gain[:, columns]
            scaled[:, columns] = value
            unit = z_abs[:, columns].astype(F32) * inverse
            total = total + jnp.sum(value * unit, axis=1, keepdims=True)
    return total / width


def second_kernel(
    slot_0, slot_1, slot_2, slot_3, z_abs, g_abs, inv, gain, mix, scale_gate, scale_lift, w_gate, w_up, down,
    keep_0, keep_1, send_0, send_1, resid,
    scaled, state, hgrad,
):
    me = lax.axis_index(AXIS)
    tokens, width = scaled.shape
    ff = hgrad.shape[1]
    inverse = inv[:, 0:1]
    mean = scaled_rows(me, (slot_0, slot_1, slot_2, slot_3), z_abs, gain, inverse, scaled)
    chunk = lane_chunk(width)
    for at in range(0, width, chunk):
        columns = slice(at, at + chunk)
        unit = z_abs[:, columns].astype(F32) * inverse
        back = (scaled[:, columns] - unit * mean) * inverse
        resid[:, columns] = back
        state[:, columns] = (g_abs[:, columns].astype(F32) + mix[:, columns] * back).astype(BF16)
    project(state, down, hgrad)
    grad = hgrad[...]
    back_project(
        (grad * scale_gate[...]).astype(BF16), (grad * scale_lift[...]).astype(BF16),
        w_gate, w_up, me, (keep_0, keep_1), (send_0, send_1),
    )


def third_kernel(
    n, slot_0, slot_1, slot_2, slot_3, z_abs, g_abs, inv, gain, mix, scale_gate, scale_lift,
    down, resid, hidden, normed,
    adjoint, d_gate, d_up, d_down,
    scaled, latest, half, hgrad, stage, sems,
):
    me = lax.axis_index(AXIS)
    tokens, width = scaled.shape
    ff = hgrad.shape[1]
    local = tokens // n
    inverse = inv[:, 0:1]
    mean = scaled_rows(me, (slot_0, slot_1, slot_2, slot_3), z_abs, gain, inverse, scaled)
    chunk = lane_chunk(width)
    cross = jnp.zeros((tokens, 1), F32)
    square = jnp.zeros((tokens, 1), F32)
    for at in range(0, width, chunk):
        columns = slice(at, at + chunk)
        unit = z_abs[:, columns].astype(F32) * inverse
        back = (scaled[:, columns] - unit * mean) * inverse
        start = g_abs[:, columns].astype(F32)
        before = resid[:, columns]
        state = start + mix[:, columns] * before
        now = start + back - state
        change = now - before
        latest[:, columns] = now
        cross = cross + jnp.sum(now * change, axis=1, keepdims=True)
        square = square + jnp.sum(change * change, axis=1, keepdims=True)
    blend = jnp.sum(cross, axis=0, keepdims=True) / (
        jnp.sum(square, axis=0, keepdims=True) + 1e-06
    )
    for at in range(0, width, chunk):
        columns = slice(at, at + chunk)
        start = g_abs[:, columns].astype(F32)
        before = resid[:, columns]
        rate = mix[:, columns]
        state = start + rate * before
        now = latest[:, columns]
        value = state - blend * (state - start) + rate * (now - blend * (now - before))
        scaled[:, columns] = value
        half[:, columns] = value.astype(BF16)
    adjoint[...] = own_rows(scaled, me, local)

    places, _, step = stage.shape
    copies = []

    def emit(left, right, target, at):
        place = len(copies) % places
        if len(copies) >= places:
            copies[-places].wait()
        stage[place] = dot_tn(left, right[:, at : at + step]).astype(BF16)
        copy = pltpu.make_async_copy(
            stage.at[place], target.at[:, pl.ds(at, step)], sems.at[place]
        )
        copy.start()
        copies.append(copy)

    for at in range(0, width, step):
        emit(hidden[...], half, d_down, at)
    project(half, down, hgrad)
    grad = hgrad[...]
    gate_grad = (grad * scale_gate[...]).astype(BF16)
    lift_grad = (grad * scale_lift[...]).astype(BF16)
    for at in range(0, width, step):
        emit(gate_grad, normed, d_gate, at)
        emit(lift_grad, normed, d_up, at)
    for copy in copies[-places:]:
        copy.wait()


def shape(dims, dtype):
    return jax.ShapeDtypeStruct(dims, dtype)


def in_hbm(array):
    return pltpu.with_memory_space_constraint(array, pltpu.HBM)


def params(state_bytes, extra=0):
    return pltpu.CompilerParams(vmem_limit_bytes=6 * 2**20 + 6 * state_bytes + extra)


def cost(flops, moved):
    return pl.CostEstimate(flops=flops, bytes_accessed=moved, transcendentals=0)


def exchange(value, n, bit):
    return lax.ppermute(value, AXIS, [(i, i ^ bit) for i in range(n)])


def add(*terms):
    total = terms[0].astype(F32)
    for term in terms[1:]:
        total = total + term.astype(F32)
    return total.astype(BF16)


def gather_slots(own, n, w_gate, w_up, w_down):
    sources = [(w_gate, "load_gate"), (w_up, "load_up")]
    ready = []
    held = own
    for stage in gather_stages(n):
        steps = stage if len(stage) == 1 else (stage[0], stage[1], stage[0] + stage[1])
        arrived = [exchange(held, n, step) for step in steps]
        if sources:
            source, name = sources.pop(0)
            ready.append(load(source, name))
            arrived, ready[-1], sources = hold_order(arrived, ready[-1], sources)
        held = jnp.concatenate([held] + arrived, axis=0)
    ready += [load(source, name) for source, name in sources]
    return held, exchange(held, n, 1), *ready, load(w_down, "load_down")


def hold_order(arrived, loaded, sources):
    names = [name for _, name in sources]
    arrived, loaded, arrays = lax.optimization_barrier((arrived, loaded, [array for array, _ in sources]))
    return arrived, loaded, list(zip(arrays, names))


def sum_everywhere(keep, send, n):
    bits = [1 << k for k in range(1, n.bit_length() - 1)]
    orders = (bits, bits[-1:] + bits[:-1])
    chunks = [add(keep[part], exchange(send[part], n, 1)) for part in range(2)]
    for step in zip(*orders):
        chunks = [add(chunk, exchange(chunk, n, bit)) for chunk, bit in zip(chunks, step)]
    others = [exchange(chunk, n, 1) for chunk in chunks]
    return chunks[0], others[0], chunks[1], others[1]


def pack(z_star, grad_out):
    local, width = z_star.shape
    return pl.pallas_call(
        pack_kernel,
        out_shape=shape((1, 2 * local, width), BF16),
        in_specs=[VMEM] * 2,
        out_specs=VMEM,
        compiler_params=params(0),
        name="pack",
    )(z_star, grad_out)


def load(weight, name):
    return pl.pallas_call(
        load_kernel,
        out_shape=shape(weight.shape, BF16),
        in_specs=[HBM],
        out_specs=VMEM,
        scratch_shapes=[pltpu.SemaphoreType.DMA((len(pieces(weight.shape[0], ROWS)),))],
        compiler_params=params(0),
        cost_estimate=cost(LOAD_FLOPS, 2 * weight.size),
        name=name,
    )(in_hbm(weight))


def call_first(n, slots_a, slots_b, gain, w_gate, w_up, w_down):
    _, packed, width = slots_a.shape
    tokens, ff = packed * n // 2, w_down.shape[0]
    partial = shape((tokens, width // 4), BF16)
    return pl.pallas_call(
        functools.partial(first_kernel, n),
        out_shape=(
            partial, partial, partial, partial,
            shape((tokens, width), BF16), shape((tokens, width), BF16), shape((tokens, 128), F32),
            shape((tokens, ff), F32), shape((tokens, ff), F32), shape((tokens, ff), BF16),
            shape((tokens, width), BF16),
        ),
        in_specs=[VMEM] * 2 + [HBM] + [VMEM] * 3,
        out_specs=(VMEM,) * 11,
        scratch_shapes=[
            pltpu.VMEM((tokens, width), F32), pltpu.VMEM((tokens, width), F32), pltpu.VMEM((1, width), F32),
            pltpu.VMEM((tokens, ff), F32), pltpu.VMEM((tokens, ff), F32), pltpu.VMEM((tokens, ff), F32),
            pltpu.SemaphoreType.DMA,
        ],
        compiler_params=params(4 * tokens * width),
        cost_estimate=cost(10 * tokens * width * ff, 6 * ff * width),
        name="first",
    )(slots_a, slots_b, in_hbm(gain), w_gate, w_up, w_down)


def call_second(slots, z_abs, g_abs, inv, gain, mix, scale_gate, scale_lift, w_gate, w_up, down):
    tokens, width = z_abs.shape
    ff = down.shape[0]
    partial = shape((tokens, width // 4), BF16)
    return pl.pallas_call(
        second_kernel,
        out_shape=(partial,) * 4 + (shape((tokens, width), F32),),
        in_specs=[VMEM] * 14,
        out_specs=(VMEM,) * 5,
        scratch_shapes=[
            pltpu.VMEM((tokens, width), F32), pltpu.VMEM((tokens, width), BF16),
            pltpu.VMEM((tokens, ff), F32),
        ],
        compiler_params=params(4 * tokens * width),
        cost_estimate=cost(6 * tokens * width * ff, 6 * ff * width),
        name="second",
    )(*slots, z_abs, g_abs, inv, gain, mix, scale_gate, scale_lift, w_gate, w_up, down)


def call_third(
    n, slots, z_abs, g_abs, inv, gain, mix, scale_gate, scale_lift, down, resid, hidden, normed
):
    tokens, width = z_abs.shape
    ff = down.shape[0]
    step = 1024 if width % 1024 == 0 else lane_chunk(width // 4)
    return pl.pallas_call(
        functools.partial(third_kernel, n),
        out_shape=(shape((tokens // n, width), F32),) + (shape((ff, width), BF16),) * 3,
        in_specs=[VMEM] * 15,
        out_specs=(VMEM, HBM, HBM, HBM),
        scratch_shapes=[
            pltpu.VMEM((tokens, width), F32), pltpu.VMEM((tokens, width), F32),
            pltpu.VMEM((tokens, width), BF16), pltpu.VMEM((tokens, ff), F32),
            pltpu.VMEM((PLACES, ff, step), BF16), pltpu.SemaphoreType.DMA((PLACES,)),
        ],
        compiler_params=params(4 * tokens * width, 2 * PLACES * ff * step),
        cost_estimate=cost(8 * tokens * width * ff, 6 * ff * width),
        name="third",
    )(*slots, z_abs, g_abs, inv, gain, mix, scale_gate, scale_lift, down, resid, hidden, normed)


def body(n, z_star, grad_out, w_gate, w_up, w_down, norm_gain, mix_rate):
    gain, mix = norm_gain[None], mix_rate[None]
    slots_a, slots_b, gate, up, down = gather_slots(pack(z_star, grad_out), n, w_gate.T, w_up.T, w_down)
    *partial, z_abs, g_abs, inv, scale_gate, scale_lift, hidden, normed = call_first(
        n, slots_a, slots_b, gain, gate, up, down
    )
    slots = sum_everywhere(partial[:2], partial[2:], n)
    *partial, resid = call_second(
        slots, z_abs, g_abs, inv, gain, mix, scale_gate, scale_lift, gate, up, down
    )
    slots = sum_everywhere(partial[:2], partial[2:], n)
    adjoint, d_gate, d_up, d_down = call_third(
        n, slots, z_abs, g_abs, inv, gain, mix, scale_gate, scale_lift, down, resid, hidden, normed
    )
    return adjoint, d_gate.T, d_up.T, d_down


def solution(mesh):
    n = mesh.shape[AXIS]
    rows = P(("group", AXIS), None)
    split = P("group", AXIS)
    placed = (rows, rows, split, split, rows, P("group"), P("group"))
    return jax.shard_map(
        functools.partial(body, n),
        mesh=mesh,
        in_specs=placed,
        out_specs=(rows, split, split, rows),
        check_vma=False,
    )
```

```python
import functools

import jax
import jax.numpy as jnp
from jax import lax
from jax.experimental import pallas as pl
from jax.experimental.pallas import tpu as pltpu
from jax.sharding import PartitionSpec as P

F32 = jnp.float32
BF16 = jnp.bfloat16
VMEM = pl.BlockSpec(memory_space=pltpu.VMEM)
HBM = pl.BlockSpec(memory_space=pltpu.HBM)
AXIS = "tensor"
ROWS = 256
LANES = 640
PLACES = 15
STREAM = 432
LOAD_FLOPS = 2 * 10**9


def dot_nn(left, right):
    return lax.dot_general(left, right, (((1,), (0,)), ((), ())), preferred_element_type=F32)


def dot_nt(left, right):
    return lax.dot_general(left, right, (((1,), (1,)), ((), ())), preferred_element_type=F32)


def dot_tn(left, right):
    return lax.dot_general(left, right, (((0,), (0,)), ((), ())), preferred_element_type=F32)


def pieces(total, size):
    return [(at, min(size, total - at)) for at in range(0, total, size)]


def lane_chunk(width):
    for size in (LANES, 512, 384, 256, 128):
        if width % size == 0:
            return size
    return width


def gather_stages(n):
    bits = [1 << k for k in reversed(range(2, n.bit_length() - 1))]
    stages = []
    while bits:
        stages.append(tuple(reversed(bits[:2])))
        bits = bits[2:]
    return stages + [(2,)]


def state_rows(slots_a, slots_b, n, me, owner):
    offset = jnp.bitwise_xor(me, owner)
    place, stride = 0, 1
    for stage in gather_stages(n):
        place = place + stride * ((offset // stage[0]) & (2 ** len(stage) - 1))
        stride *= 2 ** len(stage)
    return jnp.where((offset & 1) == 0, slots_a[place], slots_b[place])


def own_rows(ref, me, local):
    if local % 8 == 0:
        return ref[pl.ds(pl.multiple_of(me * local, 8), local), :]
    per = 8 // local
    block = ref[pl.ds(pl.multiple_of((me // per) * 8, 8), 8), :]
    value = block[:local]
    for other in range(1, per):
        value = jnp.where(me % per == other, block[other * local : (other + 1) * local], value)
    return value


def back_project(gate_grad, lift_grad, w_gate, w_up, me, part, keep, send):
    quarter = keep.shape[-1]
    for other, target in ((1, send), (0, keep)):
        at = (jnp.bitwise_xor(me & 1, other) + 2 * part) * quarter
        columns = pl.ds(pl.multiple_of(at, 128), quarter)
        value = dot_tn(gate_grad, w_gate[:, columns]) + dot_tn(lift_grad, w_up[:, columns])
        target[...] = value.astype(BF16)


def back_kernel(gate_grad, lift_grad, w_gate, w_up, keep, send):
    me = lax.axis_index(AXIS)
    back_project(gate_grad[...], lift_grad[...], w_gate, w_up, me, 1, keep, send)


def load_kernel(source, held, sems):
    copies = [
        pltpu.make_async_copy(source.at[pl.ds(at, size), :], held.at[pl.ds(at, size), :], sems.at[order])
        for order, (at, size) in enumerate(pieces(source.shape[0], ROWS))
    ]
    for copy in copies:
        copy.start()
    for copy in copies:
        copy.wait()


def pack_kernel(z, g, packed, z_rows, g_rows, sems):
    local = z_rows.shape[0]
    copies = [
        pltpu.make_async_copy(z, z_rows, sems.at[0]),
        pltpu.make_async_copy(g, g_rows, sems.at[1]),
    ]
    for copy in copies:
        copy.start()
    for copy in copies:
        copy.wait()
    packed[0, :local] = z_rows[...]
    packed[0, local:] = g_rows[...].astype(BF16)


def first_kernel(
    n, slots_a, slots_b, gain_hbm, w_gate, w_up, w_down,
    keep, send, gate_grad, lift_grad, z_abs, g_abs, inv, scale_gate, scale_lift, hidden, normed,
    z_rows, g_rows, gain, gate_pre, lifted, hgrad, gain_sem,
):
    me = lax.axis_index(AXIS)
    tokens, width = z_rows.shape
    local = tokens // n
    gain_copy = pltpu.make_async_copy(gain_hbm, gain, gain_sem)
    gain_copy.start()
    for owner in range(n):
        block = state_rows(slots_a, slots_b, n, me, owner).astype(F32)
        z_rows[owner * local : (owner + 1) * local, :] = block[:local]
        g_rows[owner * local : (owner + 1) * local, :] = block[local:]

    chunk = lane_chunk(width)
    total = jnp.zeros((tokens, 1), F32)
    for at in range(0, width, chunk):
        z = z_rows[:, at : at + chunk]
        total = total + jnp.sum(z * z, axis=1, keepdims=True)
        z_abs[:, at : at + chunk] = z.astype(BF16)
        g_abs[:, at : at + chunk] = g_rows[:, at : at + chunk].astype(BF16)
    inverse = 1.0 / jnp.sqrt(total / width + 1e-06)
    inv[...] = jnp.broadcast_to(inverse, inv.shape)
    gain_copy.wait()
    for at in range(0, width, chunk):
        unit = z_rows[:, at : at + chunk] * inverse
        normed[:, at : at + chunk] = (unit * gain[:, at : at + chunk]).astype(BF16)

    project(normed, w_gate, gate_pre)
    project(normed, w_up, lifted)
    project(g_abs, w_down, hgrad)
    pre = gate_pre[...]
    up = lifted[...]
    sigma = 1.0 / (1.0 + jnp.exp(-pre))
    gated = pre * sigma
    slope = sigma * (1.0 + pre * (1.0 - sigma))
    by_gate = up * slope
    scale_gate[...] = by_gate
    scale_lift[...] = gated
    hidden[...] = (gated * up).astype(BF16)
    grad = hgrad[...]
    by_gate_grad, by_lift_grad = (grad * by_gate).astype(BF16), (grad * gated).astype(BF16)
    gate_grad[...] = by_gate_grad
    lift_grad[...] = by_lift_grad
    back_project(by_gate_grad, by_lift_grad, w_gate, w_up, me, 0, keep, send)


def project(left, weight, target):
    for at, size in pieces(weight.shape[0], STREAM):
        target[at : at + size, :] = dot_nt(weight[at : at + size, :], left[...])


def scaled_rows(me, slots, z_abs, gain, inverse, scaled):
    quarter = slots[0].shape[-1]
    tokens, width = scaled.shape
    chunk = lane_chunk(quarter)
    total = jnp.zeros((tokens, 1), F32)
    for slot, source in enumerate(slots):
        base = jnp.bitwise_xor(me & 1, slot) * quarter
        for at in range(0, quarter, chunk):
            columns = pl.ds(pl.multiple_of(base + at, 128), chunk)
            value = source[:, at : at + chunk].astype(F32) * gain[:, columns]
            scaled[:, columns] = value
            unit = z_abs[:, columns].astype(F32) * inverse
            total = total + jnp.sum(value * unit, axis=1, keepdims=True)
    return total / width


def second_kernel(
    slot_0, slot_1, slot_2, slot_3, z_abs, g_abs, inv, gain, mix, scale_gate, scale_lift, w_gate, w_up, down,
    keep, send, gate_grad, lift_grad, resid,
    scaled, state, hgrad,
):
    me = lax.axis_index(AXIS)
    tokens, width = scaled.shape
    ff = hgrad.shape[0]
    inverse = inv[:, 0:1]
    mean = scaled_rows(me, (slot_0, slot_1, slot_2, slot_3), z_abs, gain, inverse, scaled)
    chunk = lane_chunk(width)
    for at in range(0, width, chunk):
        columns = slice(at, at + chunk)
        unit = z_abs[:, columns].astype(F32) * inverse
        back = (scaled[:, columns] - unit * mean) * inverse
        resid[:, columns] = back
        state[:, columns] = (g_abs[:, columns].astype(F32) + mix[:, columns] * back).astype(BF16)
    project(state, down, hgrad)
    grad = hgrad[...]
    by_gate_grad = (grad * scale_gate[...]).astype(BF16)
    by_lift_grad = (grad * scale_lift[...]).astype(BF16)
    gate_grad[...] = by_gate_grad
    lift_grad[...] = by_lift_grad
    back_project(by_gate_grad, by_lift_grad, w_gate, w_up, me, 0, keep, send)


def third_kernel(
    n, slot_0, slot_1, slot_2, slot_3, z_abs, g_abs, inv, gain, mix, scale_gate, scale_lift,
    down, resid, hidden, normed,
    adjoint, d_gate, d_up, d_down,
    scaled, latest, half, hgrad, stage, sems,
):
    me = lax.axis_index(AXIS)
    tokens, width = scaled.shape
    ff = hgrad.shape[0]
    local = tokens // n
    inverse = inv[:, 0:1]
    mean = scaled_rows(me, (slot_0, slot_1, slot_2, slot_3), z_abs, gain, inverse, scaled)
    chunk = lane_chunk(width)
    cross = jnp.zeros((tokens, 1), F32)
    square = jnp.zeros((tokens, 1), F32)
    for at in range(0, width, chunk):
        columns = slice(at, at + chunk)
        unit = z_abs[:, columns].astype(F32) * inverse
        back = (scaled[:, columns] - unit * mean) * inverse
        start = g_abs[:, columns].astype(F32)
        before = resid[:, columns]
        state = start + mix[:, columns] * before
        now = start + back - state
        change = now - before
        latest[:, columns] = now
        cross = cross + jnp.sum(now * change, axis=1, keepdims=True)
        square = square + jnp.sum(change * change, axis=1, keepdims=True)
    blend = jnp.sum(cross, axis=0, keepdims=True) / (
        jnp.sum(square, axis=0, keepdims=True) + 1e-06
    )
    for at in range(0, width, chunk):
        columns = slice(at, at + chunk)
        start = g_abs[:, columns].astype(F32)
        before = resid[:, columns]
        rate = mix[:, columns]
        state = start + rate * before
        now = latest[:, columns]
        value = state - blend * (state - start) + rate * (now - blend * (now - before))
        scaled[:, columns] = value
        half[:, columns] = value.astype(BF16)
    adjoint[...] = own_rows(scaled, me, local)

    places, _, step = stage.shape
    copies = []

    def emit(left, right, target, at):
        place = len(copies) % places
        if len(copies) >= places:
            copies[-places].wait()
        stage[place] = dot_nn(left, right[:, at : at + step]).astype(BF16)
        copy = pltpu.make_async_copy(
            stage.at[place], target.at[:, pl.ds(at, step)], sems.at[place]
        )
        copy.start()
        copies.append(copy)

    for at in range(0, width, step):
        emit(hidden[...], half, d_down, at)
    project(half, down, hgrad)
    grad = hgrad[...]
    gate_grad = (grad * scale_gate[...]).astype(BF16)
    lift_grad = (grad * scale_lift[...]).astype(BF16)
    for at in range(0, width, step):
        emit(gate_grad, normed, d_gate, at)
        emit(lift_grad, normed, d_up, at)
    for copy in copies[-places:]:
        copy.wait()


def shape(dims, dtype):
    return jax.ShapeDtypeStruct(dims, dtype)


def in_hbm(array):
    return pltpu.with_memory_space_constraint(array, pltpu.HBM)


def params(state_bytes, extra=0):
    return pltpu.CompilerParams(vmem_limit_bytes=6 * 2**20 + 6 * state_bytes + extra)


def cost(flops, moved):
    return pl.CostEstimate(flops=flops, bytes_accessed=moved, transcendentals=0)


def exchange(value, n, bit):
    return lax.ppermute(value, AXIS, [(i, i ^ bit) for i in range(n)])


def add(*terms):
    total = terms[0].astype(F32)
    for term in terms[1:]:
        total = total + term.astype(F32)
    return total.astype(BF16)


def gather_slots(own, n, w_gate, w_up, w_down):
    sources = [(w_gate, "load_gate"), (w_up, "load_up")]
    ready = []
    held = own
    for stage in gather_stages(n):
        steps = stage if len(stage) == 1 else (stage[0], stage[1], stage[0] + stage[1])
        arrived = [exchange(held, n, step) for step in steps]
        if sources:
            source, name = sources.pop(0)
            ready.append(load(source, name))
            arrived, ready[-1], sources = hold_order(arrived, ready[-1], sources)
        held = jnp.concatenate([held] + arrived, axis=0)
    ready += [load(source, name) for source, name in sources]
    return held, exchange(held, n, 1), *ready, load(w_down, "load_down")


def hold_order(arrived, loaded, sources):
    names = [name for _, name in sources]
    arrived, loaded, arrays = lax.optimization_barrier((arrived, loaded, [array for array, _ in sources]))
    return arrived, loaded, list(zip(arrays, names))


def sum_everywhere(keep, send, n):
    bits = [1 << k for k in range(1, n.bit_length() - 1)]
    orders = (bits[1::-1] + bits[2:], bits[-1:] + bits[:-1])
    chunks = [add(keep[part], exchange(send[part], n, 1)) for part in range(2)]
    for step in zip(*orders):
        chunks = [add(chunk, exchange(chunk, n, bit)) for chunk, bit in zip(chunks, step)]
    others = [exchange(chunk, n, 1) for chunk in chunks]
    return chunks[0], others[0], chunks[1], others[1]


def pack(z_star, grad_out):
    local, width = z_star.shape
    return pl.pallas_call(
        pack_kernel,
        out_shape=shape((1, 2 * local, width), BF16),
        in_specs=[HBM] * 2,
        out_specs=VMEM,
        scratch_shapes=[
            pltpu.VMEM((local, width), BF16), pltpu.VMEM((local, width), F32),
            pltpu.SemaphoreType.DMA((2,)),
        ],
        compiler_params=params(0),
        name="pack",
    )(in_hbm(z_star), in_hbm(grad_out))


def load(weight, name):
    return pl.pallas_call(
        load_kernel,
        out_shape=shape(weight.shape, BF16),
        in_specs=[HBM],
        out_specs=VMEM,
        scratch_shapes=[pltpu.SemaphoreType.DMA((len(pieces(weight.shape[0], ROWS)),))],
        compiler_params=params(0),
        cost_estimate=cost(LOAD_FLOPS, 2 * weight.size),
        name=name,
    )(in_hbm(weight))


def call_first(n, slots_a, slots_b, gain, w_gate, w_up, w_down):
    _, packed, width = slots_a.shape
    tokens, ff = packed * n // 2, w_down.shape[0]
    partial = shape((tokens, width // 4), BF16)
    return pl.pallas_call(
        functools.partial(first_kernel, n),
        out_shape=(
            partial, partial, shape((ff, tokens), BF16), shape((ff, tokens), BF16),
            shape((tokens, width), BF16), shape((tokens, width), BF16), shape((tokens, 128), F32),
            shape((ff, tokens), F32), shape((ff, tokens), F32), shape((ff, tokens), BF16),
            shape((tokens, width), BF16),
        ),
        in_specs=[VMEM] * 2 + [HBM] + [VMEM] * 3,
        out_specs=(VMEM,) * 11,
        scratch_shapes=[
            pltpu.VMEM((tokens, width), F32), pltpu.VMEM((tokens, width), F32), pltpu.VMEM((1, width), F32),
            pltpu.VMEM((ff, tokens), F32), pltpu.VMEM((ff, tokens), F32), pltpu.VMEM((ff, tokens), F32),
            pltpu.SemaphoreType.DMA,
        ],
        compiler_params=params(4 * tokens * width),
        cost_estimate=cost(10 * tokens * width * ff, 6 * ff * width),
        name="first",
    )(slots_a, slots_b, in_hbm(gain), w_gate, w_up, w_down)


def call_back(gate_grad, lift_grad, w_gate, w_up):
    ff, tokens = gate_grad.shape
    width = w_gate.shape[1]
    partial = shape((tokens, width // 4), BF16)
    return pl.pallas_call(
        back_kernel,
        out_shape=(partial, partial),
        in_specs=[VMEM] * 4,
        out_specs=(VMEM,) * 2,
        compiler_params=params(4 * tokens * width),
        cost_estimate=cost(LOAD_FLOPS, 2 * ff * width),
        name="back",
    )(gate_grad, lift_grad, w_gate, w_up)


def call_second(slots, z_abs, g_abs, inv, gain, mix, scale_gate, scale_lift, w_gate, w_up, down):
    tokens, width = z_abs.shape
    ff = down.shape[0]
    partial = shape((tokens, width // 4), BF16)
    return pl.pallas_call(
        second_kernel,
        out_shape=(partial,) * 2 + (shape((ff, tokens), BF16),) * 2 + (shape((tokens, width), F32),),
        in_specs=[VMEM] * 14,
        out_specs=(VMEM,) * 5,
        scratch_shapes=[
            pltpu.VMEM((tokens, width), F32), pltpu.VMEM((tokens, width), BF16),
            pltpu.VMEM((ff, tokens), F32),
        ],
        compiler_params=params(4 * tokens * width),
        cost_estimate=cost(6 * tokens * width * ff, 6 * ff * width),
        name="second",
    )(*slots, z_abs, g_abs, inv, gain, mix, scale_gate, scale_lift, w_gate, w_up, down)


def call_third(
    n, slots, z_abs, g_abs, inv, gain, mix, scale_gate, scale_lift, down, resid, hidden, normed
):
    tokens, width = z_abs.shape
    ff = down.shape[0]
    step = 1024 if width % 1024 == 0 else lane_chunk(width // 4)
    return pl.pallas_call(
        functools.partial(third_kernel, n),
        out_shape=(shape((tokens // n, width), F32),) + (shape((ff, width), BF16),) * 3,
        in_specs=[VMEM] * 15,
        out_specs=(VMEM, HBM, HBM, HBM),
        scratch_shapes=[
            pltpu.VMEM((tokens, width), F32), pltpu.VMEM((tokens, width), F32),
            pltpu.VMEM((tokens, width), BF16), pltpu.VMEM((ff, tokens), F32),
            pltpu.VMEM((PLACES, ff, step), BF16), pltpu.SemaphoreType.DMA((PLACES,)),
        ],
        compiler_params=params(4 * tokens * width, 2 * PLACES * ff * step),
        cost_estimate=cost(8 * tokens * width * ff, 6 * ff * width),
        name="third",
    )(*slots, z_abs, g_abs, inv, gain, mix, scale_gate, scale_lift, down, resid, hidden, normed)


def body(n, z_star, grad_out, w_gate, w_up, w_down, norm_gain, mix_rate):
    gain, mix = norm_gain[None], mix_rate[None]
    slots_a, slots_b, gate, up, down = gather_slots(pack(z_star, grad_out), n, w_gate.T, w_up.T, w_down)
    keep, send, gate_grad, lift_grad, z_abs, g_abs, inv, scale_gate, scale_lift, hidden, normed = call_first(
        n, slots_a, slots_b, gain, gate, up, down
    )
    late = call_back(gate_grad, lift_grad, gate, up)
    slots = sum_everywhere((keep, late[0]), (send, late[1]), n)
    keep, send, gate_grad, lift_grad, resid = call_second(
        slots, z_abs, g_abs, inv, gain, mix, scale_gate, scale_lift, gate, up, down
    )
    late = call_back(gate_grad, lift_grad, gate, up)
    slots = sum_everywhere((keep, late[0]), (send, late[1]), n)
    adjoint, d_gate, d_up, d_down = call_third(
        n, slots, z_abs, g_abs, inv, gain, mix, scale_gate, scale_lift, down, resid, hidden, normed
    )
    return adjoint, d_gate.T, d_up.T, d_down


def solution(mesh):
    n = mesh.shape[AXIS]
    rows = P(("group", AXIS), None)
    split = P("group", AXIS)
    placed = (rows, rows, split, split, rows, P("group"), P("group"))
    return jax.shard_map(
        functools.partial(body, n),
        mesh=mesh,
        in_specs=placed,
        out_specs=(rows, split, split, rows),
        check_vma=False,
    )
```
